256 devices in a mesh: rows: 128 (over y, x, z), cols: 2 (over core).
Axes of the slice: x: 4, y: 4, z: 8, core: 2. Of those that a mesh axis runs over, the one named last changes fastest.
Arguments:
- points: float32 [65536, 768], P('rows'), may hold values from -83 to 83
- landmark_index: int32 [32768], P('rows'), may hold values from 0 to 65535, as said below
- targets: float32 [32768, 512], P('rows', 'cols'), may hold values from -6 to 6
- ridge_shift: float32 [1], replicated, may hold values from 0.5 to 2
Outputs:
- projected: float32 [512, 2048], P('rows', 'cols')
- panels: float32 [32768, 256], P('rows')
- remainder: float32 [32768, 1792], P('rows', 'cols')
The draws below stay inside these ranges and needn't reach their ends.
Inputs may be any that keep to these rules, and one draw needn't show every extreme that they name: `landmark_index`: landmark i is a point of the block [(i // 256) * 512, (i // 256 + 1) * 512); the 256 landmarks of one block are distinct.
All inputs are finite; a program needn't handle non-finite values.
Results may differ from the reference program's by a relative error of at most 0.00028.
Values sent between devices are 32-bit elements; how exact they have to be, the bound alone decides.
No kernel may reach another device: no remote copies, remote signals or barrier semaphores. Data moves between devices by JAX's collectives and lax.ppermute only.
A program may use at most 64 MiB of HBM per device.

```python
import math
import jax
import jax.numpy as jnp
from jax import lax

E = 768
C = 2048
R = 512
PW = 128
L_DEV = 256
P_DEV = 512
LANDMARKS = 32768
POINTS = 65536
N_ROWS = 128


def draw_landmark_index(key, part):
    blocks = LANDMARKS // L_DEV
    block_keys = jax.random.split(jax.random.fold_in(key, 17), blocks)
    chosen = jax.vmap(lambda block_key: jax.random.permutation(block_key, P_DEV)[:L_DEV])(block_keys)
    shifted = chosen + (jnp.arange(blocks, dtype=jnp.int32) * P_DEV)[:, None]
    return shifted.reshape(-1).astype(jnp.int32)


def draw_points(key, part):
    base_key = jax.random.fold_in(key, 29)
    latent_key, mapping_key, perturb_key = jax.random.split(base_key, 3)
    mapping = jnp.clip(jax.random.normal(mapping_key, (8, E), jnp.float32) * math.sqrt(3.0 / 8.0), -2.5, 2.5)
    latent = jnp.clip(jax.random.normal(latent_key, (POINTS, 8), jnp.float32), -4.0, 4.0)
    perturb = 0.3 * jnp.clip(jax.random.normal(perturb_key, (POINTS, E), jnp.float32), -4.0, 4.0)
    mapped = jnp.dot(latent, mapping, precision=lax.Precision.HIGHEST, preferred_element_type=jnp.float32)
    return (mapped + perturb).astype(jnp.float32)


def steps_of(stream_key, dims, pieces, smallest, high):
    gain = 1.0
    for position, blocks in pieces:
        heights = jax.random.uniform(jax.random.fold_in(jax.random.fold_in(stream_key, 6), position), (blocks,), jnp.float32, smallest / len(pieces), high / len(pieces))
        gain = gain * jnp.repeat(jnp.exp(heights), dims[position] // blocks).reshape((-1,) + (1,) * (len(dims) - 1 - position))
    return gain


def centred(rng, extent, scale, most, shards=(), kind=jnp.bfloat16):
    drawn = scale * jax.random.normal(rng, extent, jnp.float32)
    if shards:
        drawn = drawn * steps_of(rng, extent, shards, -0.22, 0.18)
    return jnp.clip(drawn, -most, most).astype(kind)


def setup_inputs(seed: int = 0) -> dict:
    splits = jax.random.split(jax.random.key(seed), 5)
    return {
        "points": draw_points(jax.random.fold_in(splits[4], 71), 0),
        "landmark_index": draw_landmark_index(jax.random.fold_in(splits[4], 71), 0),
        "targets": centred(splits[2], (LANDMARKS, R), 1.0, 6.0, ((0, 128), (1, 2)), jnp.float32),
        "ridge_shift": jnp.clip(jnp.exp(jax.random.uniform(splits[3], (1,), jnp.float32, math.log(0.5), math.log(2.0))), 0.5, 2.0),
    }


exact_mode = lax.Precision.HIGHEST

def gaussian(left_rows, right_rows):
    left_sq = jnp.sum(left_rows * left_rows, axis=1)
    right_sq = jnp.sum(right_rows * right_rows, axis=1)
    cross_term = jnp.dot(left_rows.astype(jnp.float32), right_rows.T.astype(jnp.float32), precision=exact_mode, preferred_element_type=jnp.float32)
    return jnp.exp(-(left_sq[:, None] + right_sq[None, :] - 2.0 * cross_term) / (2.0 * left_rows.shape[1]))

def reference(points, landmark_index, targets, ridge_shift):
    embedded = points[landmark_index]
    half_cols = C // 2
    quarter = half_cols // N_ROWS
    column_ids = jnp.arange(C, dtype=jnp.int32)
    within = column_ids % half_cols
    land_cols = within // quarter * L_DEV + column_ids // half_cols * quarter + within % quarter
    column_emb = embedded[land_cols]
    row_ids = jnp.arange(embedded.shape[0], dtype=jnp.int32)
    kernel_slab = gaussian(embedded, column_emb) + jnp.where(row_ids[:, None] == land_cols[None, :], ridge_shift[0], 0.0)
    projected = lax.dot_general(targets.astype(jnp.float32), kernel_slab.astype(jnp.float32), (((0,), (0,)), ((), ())), precision=exact_mode, preferred_element_type=jnp.float32)
    panel_list = []
    for first_col in (0, half_cols):
        panel_cols = kernel_slab[:, first_col:first_col + PW]
        diag_block = panel_cols[land_cols[first_col:first_col + PW]]
        factor = jnp.linalg.cholesky(diag_block)
        local_panel = jax.scipy.linalg.solve_triangular(factor, panel_cols.T, lower=True).T
        kernel_slab = kernel_slab - jnp.dot(local_panel.astype(jnp.float32), local_panel[land_cols].T.astype(jnp.float32), precision=exact_mode, preferred_element_type=jnp.float32)
        panel_list.append(local_panel)
    remainder = jnp.concatenate([kernel_slab[:, PW:half_cols], kernel_slab[:, half_cols + PW:]], axis=1)
    return (projected, jnp.concatenate(panel_list, axis=1), remainder)
```

```python
import jax
import jax.numpy as jnp
from jax import lax
from jax.sharding import Mesh
from jax.sharding import PartitionSpec as P

C = 2048
PW = 128
ROWS = ("rows_0", "rows_1", "rows_2")
PLANE = ("rows_0", "rows_1")

exact_mode = lax.Precision.HIGHEST


def to_all(x, axis):
    peers = lax.axis_size(axis)
    return lax.all_to_all(jnp.broadcast_to(x[None], (peers, *x.shape)), axis, 0, 0, tiled=True)


def summed(x, axis):
    peers = lax.axis_size(axis)
    pieces = x.reshape(peers, x.shape[0] // peers, *x.shape[1:])
    return lax.all_to_all(pieces, axis, 0, 0, tiled=True).sum(axis=0)


def dot_t(left, right):
    return lax.dot_general(
        left, right, (((1,), (1,)), ((), ())), precision=exact_mode, preferred_element_type=jnp.float32
    )


def gaussian(left, left_sq, right, right_sq):
    cross = dot_t(left, right)
    return jnp.exp(-(left_sq[:, None] + right_sq[None, :] - 2.0 * cross) / (2.0 * left.shape[1]))


def squares(x):
    return jnp.sum(x * x, axis=1)


def lower_inverse(block):
    factor = jnp.linalg.cholesky(block)
    eye = jnp.eye(PW, dtype=jnp.float32)
    return jax.scipy.linalg.solve_triangular(factor, eye, lower=True)


def per_device(points, landmark_index, targets, ridge_shift):
    rows_here = landmark_index.shape[0]
    block_points = points.shape[0]
    row_pos = lax.axis_index(ROWS)
    col_pos = lax.axis_index("cols")
    n_rows = lax.axis_size(ROWS)
    half_cols = C // 2
    quarter = half_cols // n_rows
    ridge = ridge_shift[0]

    peer_targets = lax.ppermute(targets, "cols", [(0, 1), (1, 0)])
    first = col_pos == 0
    all_targets = jnp.concatenate(
        [jnp.where(first, targets, peer_targets), jnp.where(first, peer_targets, targets)], axis=1
    )

    embedded = jnp.take(points, landmark_index - row_pos * block_points, axis=0)
    own = lax.dynamic_slice_in_dim(embedded, col_pos * quarter, quarter, 0)
    column_emb = to_all(to_all(own, "rows_2"), PLANE).reshape(half_cols, -1)

    emb_sq = squares(embedded)
    col_sq = squares(column_emb)
    row_ids = lax.broadcasted_iota(jnp.int32, (rows_here, half_cols), 0)
    col_ids = lax.broadcasted_iota(jnp.int32, (rows_here, half_cols), 1)
    offset = row_ids - col_pos * quarter
    ridge_hits = (offset >= 0) & (offset < quarter) & (col_ids == row_pos * quarter + offset)
    slab = gaussian(embedded, emb_sq, column_emb, col_sq) + jnp.where(ridge_hits, ridge, 0.0)

    partial = lax.dot_general(
        all_targets, slab, (((0,), (0,)), ((), ())), precision=exact_mode, preferred_element_type=jnp.float32
    )
    projected = summed(summed(partial, PLANE), "rows_2")

    own_heads = column_emb[:PW]
    peer_heads = lax.ppermute(own_heads, "cols", [(0, 1), (1, 0)])
    heads = jnp.concatenate(
        [jnp.where(first, own_heads, peer_heads), jnp.where(first, peer_heads, own_heads)], axis=0
    )
    heads_sq = squares(heads)

    def at_heads(emb, emb_sq, landmark):
        base = gaussian(emb, emb_sq, heads, heads_sq)
        head = lax.broadcasted_iota(jnp.int32, base.shape, 1)
        block, within = head // PW, head % PW
        place = within // quarter * rows_here + block * quarter + within % quarter
        return base + jnp.where(place == landmark[:, None], ridge, 0.0)

    here = row_pos * rows_here + lax.iota(jnp.int32, rows_here)
    column = lax.iota(jnp.int32, half_cols)
    there = column // quarter * rows_here + col_pos * quarter + column % quarter
    head = lax.iota(jnp.int32, 2 * PW)
    head_place = head % PW // quarter * rows_here + head // PW * quarter + head % quarter
    rows_local = at_heads(embedded, emb_sq, here)
    rows_column = at_heads(column_emb, col_sq, there)
    block = at_heads(heads, heads_sq, head_place)

    inv_0 = lower_inverse(block[:PW, :PW])
    corner = dot_t(block[PW:, :PW], inv_0)
    inv_1 = lower_inverse(block[PW:, PW:] - dot_t(corner, corner))

    def panels_of(rows):
        left = dot_t(rows[:, :PW], inv_0)
        right = dot_t(rows[:, PW:] - dot_t(left, corner), inv_1)
        return jnp.concatenate([left, right], axis=1)

    panels = panels_of(rows_local)
    at_columns = panels_of(rows_column[PW:])
    remainder = slab[:, PW:] - dot_t(panels, at_columns)
    return projected, panels, remainder


def solution(mesh):
    split = Mesh(
        mesh.devices.reshape(4, 4, 8, mesh.shape["cols"]), ("rows_0", "rows_1", "rows_2", "cols")
    )
    placed = (P(ROWS, None), P(ROWS), P(ROWS, "cols"), P())
    return jax.shard_map(
        per_device,
        mesh=split,
        in_specs=placed,
        out_specs=(P(ROWS, "cols"), P(ROWS, None), P(ROWS, "cols")),
        check_vma=False,
    )
```

```python
import jax
import jax.numpy as jnp
from jax import lax
from jax.experimental import pallas as pl
from jax.sharding import Mesh
from jax.sharding import PartitionSpec as P

C = 2048
PW = 128
ROWS = ("rows_0", "rows_1", "rows_2")
PLANE = ("rows_0", "rows_1")
SUB = 8

exact_mode = lax.Precision.HIGHEST


def to_all(x, axis):
    peers = lax.axis_size(axis)
    return lax.all_to_all(jnp.broadcast_to(x[None], (peers, *x.shape)), axis, 0, 0, tiled=True)


def summed(x, axis):
    peers = lax.axis_size(axis)
    pieces = x.reshape(peers, x.shape[0] // peers, *x.shape[1:])
    return lax.all_to_all(pieces, axis, 0, 0, tiled=True).sum(axis=0)


def dot_t(left, right):
    return lax.dot_general(
        left, right, (((1,), (1,)), ((), ())), precision=exact_mode, preferred_element_type=jnp.float32
    )


def gaussian(left, left_sq, right, right_sq):
    cross = dot_t(left, right)
    return jnp.exp(-(left_sq[:, None] + right_sq[None, :] - 2.0 * cross) / (2.0 * left.shape[1]))


def squares(x):
    return jnp.sum(x * x, axis=1)


def inverse_factor(rows):
    groups = len(rows)
    ids = lax.broadcasted_iota(jnp.int32, (SUB, PW), 0)
    lanes = lax.broadcasted_iota(jnp.int32, (SUB, PW), 1)
    inv = [jnp.where(lanes == ids + SUB * g, 1.0, 0.0).astype(jnp.float32) for g in range(groups)]
    for b in range(groups):
        cols = [
            [jnp.broadcast_to(rows[i][:, SUB * b + j : SUB * b + j + 1], (SUB, PW)) for i in range(b, groups)]
            for j in range(SUB)
        ]
        head, inv_head = rows[b], inv[b]
        steps = []
        for k in range(SUB):
            spread = [jnp.broadcast_to(cols[k][0][j : j + 1], (SUB, PW)) for j in range(k, SUB)]
            scale = lax.rsqrt(spread[0])
            row = jnp.broadcast_to(head[k : k + 1], (SUB, PW)) * scale
            inv_row = jnp.broadcast_to(inv_head[k : k + 1], (SUB, PW)) * scale
            mult = [c * scale for c in cols[k]]
            mult[0] = jnp.where(ids > k, mult[0], 0.0)
            for j in range(k + 1, SUB):
                there = spread[j - k] * scale
                cols[j] = [c - m * there for c, m in zip(cols[j], mult)]
            head = head - mult[0] * row
            inv_head = jnp.where(ids == k, inv_row, inv_head - mult[0] * inv_row)
            steps.append((row, inv_row, mult))
        inv[b] = inv_head
        for i in range(b + 1, groups):
            for row, inv_row, mult in steps:
                rows[i] = rows[i] - mult[i - b] * row
                inv[i] = inv[i] - mult[i - b] * inv_row
    return inv


def factor_kernel(block_ref, first_ref, corner_ref, second_ref):
    def factor_into(block, out_ref):
        inv = inverse_factor([block[SUB * g : SUB * g + SUB] for g in range(PW // SUB)])
        for g, rows in enumerate(inv):
            out_ref[SUB * g : SUB * g + SUB, :] = rows

    factor_into(block_ref[:PW, :PW], first_ref)
    corner = dot_t(block_ref[PW:, :PW], first_ref[...])
    corner_ref[...] = corner
    factor_into(block_ref[PW:, PW:] - dot_t(corner, corner), second_ref)


def factors(block):
    shape = jax.ShapeDtypeStruct((PW, PW), jnp.float32)
    return pl.pallas_call(
        factor_kernel,
        out_shape=(shape,) * 3,
        cost_estimate=pl.CostEstimate(flops=20_000_000, bytes_accessed=500_000, transcendentals=256),
    )(block)


def per_device(points, landmark_index, targets, ridge_shift):
    rows_here = landmark_index.shape[0]
    block_points = points.shape[0]
    row_pos = lax.axis_index(ROWS)
    col_pos = lax.axis_index("cols")
    n_rows = lax.axis_size(ROWS)
    half_cols = C // 2
    quarter = half_cols // n_rows
    ridge = ridge_shift[0]

    peer_targets = lax.ppermute(targets, "cols", [(0, 1), (1, 0)])
    first = col_pos == 0
    all_targets = jnp.concatenate(
        [jnp.where(first, targets, peer_targets), jnp.where(first, peer_targets, targets)], axis=1
    )

    embedded = jnp.take(points, landmark_index - row_pos * block_points, axis=0)
    own = lax.dynamic_slice_in_dim(embedded, col_pos * quarter, quarter, 0)
    column_emb = to_all(to_all(own, "rows_2"), PLANE).reshape(half_cols, -1)

    emb_sq = squares(embedded)
    col_sq = squares(column_emb)
    row_ids = lax.broadcasted_iota(jnp.int32, (rows_here, half_cols), 0)
    col_ids = lax.broadcasted_iota(jnp.int32, (rows_here, half_cols), 1)
    offset = row_ids - col_pos * quarter
    ridge_hits = (offset >= 0) & (offset < quarter) & (col_ids == row_pos * quarter + offset)
    slab = gaussian(embedded, emb_sq, column_emb, col_sq) + jnp.where(ridge_hits, ridge, 0.0)

    partial = lax.dot_general(
        all_targets, slab, (((0,), (0,)), ((), ())), precision=exact_mode, preferred_element_type=jnp.float32
    )
    projected = summed(summed(partial, PLANE), "rows_2")

    own_heads = column_emb[:PW]
    peer_heads = lax.ppermute(own_heads, "cols", [(0, 1), (1, 0)])
    heads = jnp.concatenate(
        [jnp.where(first, own_heads, peer_heads), jnp.where(first, peer_heads, own_heads)], axis=0
    )
    heads_sq = squares(heads)

    def at_heads(emb, emb_sq, landmark):
        base = gaussian(emb, emb_sq, heads, heads_sq)
        head = lax.broadcasted_iota(jnp.int32, base.shape, 1)
        block, within = head // PW, head % PW
        place = within // quarter * rows_here + block * quarter + within % quarter
        return base + jnp.where(place == landmark[:, None], ridge, 0.0)

    here = row_pos * rows_here + lax.iota(jnp.int32, rows_here)
    column = lax.iota(jnp.int32, half_cols)
    there = column // quarter * rows_here + col_pos * quarter + column % quarter
    head = lax.iota(jnp.int32, 2 * PW)
    head_place = head % PW // quarter * rows_here + head // PW * quarter + head % quarter
    rows_local = at_heads(embedded, emb_sq, here)
    rows_column = at_heads(column_emb, col_sq, there)
    block = at_heads(heads, heads_sq, head_place)

    inv_0, corner, inv_1 = factors(block)

    def panels_of(rows):
        left = dot_t(rows[:, :PW], inv_0)
        right = dot_t(rows[:, PW:] - dot_t(left, corner), inv_1)
        return jnp.concatenate([left, right], axis=1)

    panels = panels_of(rows_local)
    at_columns = panels_of(rows_column[PW:])
    remainder = slab[:, PW:] - dot_t(panels, at_columns)
    return projected, panels, remainder


def solution(mesh):
    split = Mesh(
        mesh.devices.reshape(4, 4, 8, mesh.shape["cols"]), ("rows_0", "rows_1", "rows_2", "cols")
    )
    placed = (P(ROWS, None), P(ROWS), P(ROWS, "cols"), P())
    return jax.shard_map(
        per_device,
        mesh=split,
        in_specs=placed,
        out_specs=(P(ROWS, "cols"), P(ROWS, None), P(ROWS, "cols")),
        check_vma=False,
    )
```

```python
import jax
import jax.numpy as jnp
from jax import lax
from jax.experimental import pallas as pl
from jax.experimental.pallas import tpu as pltpu
from jax.sharding import Mesh
from jax.sharding import PartitionSpec as P


C = 2048
PW = 128
Y = ("half", "near")
PLANE = ("half", "near", "x")
NEAR = ("near", "x")
ROWS = ("half", "near", "x", "z")
SUB = 8

exact_mode = lax.Precision.HIGHEST


def to_all(x, axis):
    peers = lax.axis_size(axis)
    return lax.all_to_all(jnp.broadcast_to(x[None], (peers, *x.shape)), axis, 0, 0, tiled=True)


def dot_t(left, right):
    return lax.dot_general(
        left, right, (((1,), (1,)), ((), ())), precision=exact_mode, preferred_element_type=jnp.float32
    )


def gaussian(left, left_sq, right, right_sq):
    cross = dot_t(left, right)
    return jnp.exp(-(left_sq[:, None] + right_sq[None, :] - 2.0 * cross) / (2.0 * left.shape[1]))


def squares(x):
    return jnp.sum(x * x, axis=1)


def inverse_factor(rows):
    groups = len(rows)
    ids = lax.broadcasted_iota(jnp.int32, (SUB, PW), 0)
    lanes = lax.broadcasted_iota(jnp.int32, (SUB, PW), 1)
    inv = [jnp.where(lanes == ids + SUB * g, 1.0, 0.0).astype(jnp.float32) for g in range(groups)]
    for b in range(groups):
        cols = [
            [jnp.broadcast_to(rows[i][:, SUB * b + j : SUB * b + j + 1], (SUB, PW)) for i in range(b, groups)]
            for j in range(SUB)
        ]
        head, inv_head = rows[b], inv[b]
        steps = []
        for k in range(SUB):
            spread = [jnp.broadcast_to(cols[k][0][j : j + 1], (SUB, PW)) for j in range(k, SUB)]
            scale = lax.rsqrt(spread[0])
            row = jnp.broadcast_to(head[k : k + 1], (SUB, PW)) * scale
            inv_row = jnp.broadcast_to(inv_head[k : k + 1], (SUB, PW)) * scale
            mult = [c * scale for c in cols[k]]
            mult[0] = jnp.where(ids > k, mult[0], 0.0)
            for j in range(k + 1, SUB):
                there = spread[j - k] * scale
                cols[j] = [c - m * there for c, m in zip(cols[j], mult)]
            head = head - mult[0] * row
            inv_head = jnp.where(ids == k, inv_row, inv_head - mult[0] * inv_row)
            steps.append((row, inv_row, mult))
        inv[b] = inv_head
        for i in range(b + 1, groups):
            for row, inv_row, mult in steps:
                rows[i] = rows[i] - mult[i - b] * row
                inv[i] = inv[i] - mult[i - b] * inv_row
    return inv


def update_kernel(block_ref, rows_ref, cols_ref, tile_ref, panel_ref, mine_ref, given_ref, first_ref, second_ref):
    def factor_into(block, out_ref):
        inv = inverse_factor([block[SUB * g : SUB * g + SUB] for g in range(PW // SUB)])
        for g, rows in enumerate(inv):
            out_ref[SUB * g : SUB * g + SUB, :] = rows

    factor_into(block_ref[:PW, :PW], first_ref)
    corner = dot_t(block_ref[PW:, :PW], first_ref[...])
    factor_into(block_ref[PW:, PW:] - dot_t(corner, corner), second_ref)

    def panels_of(ref):
        left = dot_t(ref[:, :PW], first_ref[...])
        return left, dot_t(ref[:, PW:] - dot_t(left, corner), second_ref[...])

    row_left, row_right = panels_of(rows_ref)
    col_left, col_right = panels_of(cols_ref)
    kept = panel_ref.shape[0]
    panel_ref[:, :PW] = row_left[:kept]
    panel_ref[:, PW:] = row_right[:kept]
    for out_ref, start in ((given_ref, kept), (mine_ref, 0)):
        part = slice(start, start + kept)
        out_ref[...] = (
            tile_ref[part, :] - dot_t(row_left[part], col_left) - dot_t(row_right[part], col_right)
        )


def updated(block, rows, cols, tile):
    kept = rows.shape[0] // 2
    wide = jax.ShapeDtypeStruct((kept, tile.shape[1]), jnp.float32)
    return pl.pallas_call(
        update_kernel,
        out_shape=(jax.ShapeDtypeStruct((kept, 2 * PW), jnp.float32), wide, wide),
        scratch_shapes=[pltpu.VMEM((PW, PW), jnp.float32)] * 2,
        cost_estimate=pl.CostEstimate(flops=400_000_000, bytes_accessed=4_000_000, transcendentals=256),
    )(block, rows, cols, tile)


def per_device(points, landmark_index, targets, ridge_shift):
    rows_here = landmark_index.shape[0]
    block_points = points.shape[0]
    row_pos = lax.axis_index(ROWS)
    col_pos = lax.axis_index("cols")
    y_pos = lax.axis_index(Y)
    n_rows = lax.axis_size(ROWS)
    n_y = lax.axis_size(Y)
    per_y = n_rows // n_y
    quarter = C // 2 // n_rows
    half = C // 4
    half_pos = lax.axis_index("half")
    upper = half_pos == 1
    ridge = ridge_shift[0]
    across = [(y, n_y - 1 - y) for y in range(n_y)]
    swap = [(0, 1), (1, 0)]

    def ordered(flag, mine, other, axis):
        return jnp.concatenate([jnp.where(flag, other, mine), jnp.where(flag, mine, other)], axis=axis)

    embedded = jnp.take(points, landmark_index - row_pos * block_points, axis=0)
    own = lax.dynamic_slice_in_dim(embedded, col_pos * quarter, quarter, 0)
    peer_embedded = lax.ppermute(embedded, Y, across)
    own_line = to_all(own, "z")
    column_emb = to_all(own_line, NEAR).reshape(half, -1)
    own_targets = jnp.concatenate([targets, lax.ppermute(targets, Y, across)], axis=0)
    pair_targets = ordered(col_pos == 1, own_targets, lax.ppermute(own_targets, "cols", swap), 1)
    rows_emb = jnp.concatenate([embedded, peer_embedded], axis=0)

    rows_sq = squares(rows_emb)
    col_sq = squares(column_emb)
    peer_pos = row_pos + (n_y - 1 - 2 * y_pos) * per_y
    local = lax.iota(jnp.int32, rows_here)
    row_place = jnp.concatenate([row_pos * rows_here + local, peer_pos * rows_here + local])
    column = half_pos * half + lax.iota(jnp.int32, half)
    col_place = column // quarter * rows_here + col_pos * quarter + column % quarter

    tile = gaussian(rows_emb, rows_sq, column_emb, col_sq)
    tile = tile + jnp.where(row_place[:, None] == col_place[None, :], ridge, 0.0)
    partial = lax.dot_general(
        pair_targets, tile, (((0,), (0,)), ((), ())), precision=exact_mode, preferred_element_type=jnp.float32
    )
    n_plane = lax.axis_size(PLANE)
    n_z = lax.axis_size("z")
    arrived = lax.all_to_all(partial.reshape(n_plane, -1, half), PLANE, 0, 0, tiled=True)
    nearer = arrived.reshape(2, n_plane // 2, -1, half).sum(axis=1)
    nearer = nearer.reshape(2, n_z, -1, half).swapaxes(0, 1)
    projected = lax.all_to_all(nearer, "z", 0, 0, tiled=True).sum(axis=0)
    projected = jnp.concatenate([projected[0], projected[1]], axis=1)

    sent_heads = lax.ppermute(column_emb[:PW], Y, [(y, n_y - 1 - y) for y in range(n_y // 2)])
    own_heads = jnp.where(upper, sent_heads, column_emb[:PW])
    heads = ordered(col_pos == 1, own_heads, lax.ppermute(own_heads, "cols", swap), 0)
    heads_sq = squares(heads)
    head = lax.iota(jnp.int32, 2 * PW)
    head_place = head % PW // quarter * rows_here + head // PW * quarter + head % quarter

    def at_heads(emb, emb_sq, place):
        base = gaussian(emb, emb_sq, heads, heads_sq)
        return base + jnp.where(place[:, None] == head_place[None, :], ridge, 0.0)

    operands = (
        at_heads(heads, heads_sq, head_place),
        at_heads(rows_emb, rows_sq, row_place),
        at_heads(column_emb, col_sq, col_place),
        tile,
    )
    panels, mine, given = updated(*operands)
    taken = lax.ppermute(given, Y, across)
    remainder = jnp.concatenate(
        [jnp.where(upper, taken, mine)[:, PW:], jnp.where(upper, mine, taken)], axis=1
    )
    return projected, panels, remainder


def solution(mesh):
    split = Mesh(
        mesh.devices.reshape(2, 2, 4, 8, mesh.shape["cols"]), ("half", "near", "x", "z", "cols")
    )
    placed = (P(ROWS, None), P(ROWS), P(ROWS, "cols"), P())
    return jax.shard_map(
        per_device,
        mesh=split,
        in_specs=placed,
        out_specs=(P(ROWS, "cols"), P(ROWS, None), P(ROWS, "cols")),
        check_vma=False,
    )
```

```python
import jax
import jax.numpy as jnp
from jax import lax
from jax.experimental import pallas as pl
from jax.experimental.pallas import tpu as pltpu
from jax.sharding import Mesh
from jax.sharding import PartitionSpec as P


C = 2048
PW = 128
Y = ("half", "near")
PLANE = ("half", "near", "x")
NEAR = ("near", "x")
ROWS = ("half", "near", "x", "z")
SUB = 8

exact_mode = lax.Precision.HIGHEST


def to_all(x, axis):
    peers = lax.axis_size(axis)
    return lax.all_to_all(jnp.broadcast_to(x[None], (peers, *x.shape)), axis, 0, 0, tiled=True)


def dot_t(left, right):
    return lax.dot_general(
        left, right, (((1,), (1,)), ((), ())), precision=exact_mode, preferred_element_type=jnp.float32
    )


def in_two(x):
    high = x.astype(jnp.bfloat16)
    return high, (x - high.astype(jnp.float32)).astype(jnp.bfloat16)


def split_dot_t(left, right):
    def part(a, b):
        return lax.dot_general(a, b, (((1,), (1,)), ((), ())), preferred_element_type=jnp.float32)

    return part(left[0], right[1]) + part(left[1], right[0]) + part(left[0], right[0])


def gaussian(left, left_sq, right, right_sq):
    cross = dot_t(left, right)
    return jnp.exp(-(left_sq[:, None] + right_sq[None, :] - 2.0 * cross) / (2.0 * left.shape[1]))


def squares(x):
    return jnp.sum(x * x, axis=1)


def inverse_factor(rows):
    groups = len(rows)
    ids = lax.broadcasted_iota(jnp.int32, (SUB, PW), 0)
    lanes = lax.broadcasted_iota(jnp.int32, (SUB, PW), 1)
    inv = [jnp.where(lanes == ids + SUB * g, 1.0, 0.0).astype(jnp.float32) for g in range(groups)]
    for b in range(groups):
        cols = [
            [jnp.broadcast_to(rows[i][:, SUB * b + j : SUB * b + j + 1], (SUB, PW)) for i in range(b, groups)]
            for j in range(SUB)
        ]
        head, inv_head = rows[b], inv[b]
        steps = []
        for k in range(SUB):
            spread = [jnp.broadcast_to(cols[k][0][j : j + 1], (SUB, PW)) for j in range(k, SUB)]
            scale = lax.rsqrt(spread[0])
            row = jnp.broadcast_to(head[k : k + 1], (SUB, PW)) * scale
            inv_row = jnp.broadcast_to(inv_head[k : k + 1], (SUB, PW)) * scale
            mult = [c * scale for c in cols[k]]
            mult[0] = jnp.where(ids > k, mult[0], 0.0)
            for j in range(k + 1, SUB):
                there = spread[j - k] * scale
                cols[j] = [c - m * there for c, m in zip(cols[j], mult)]
            head = head - mult[0] * row
            inv_head = jnp.where(ids == k, inv_row, inv_head - mult[0] * inv_row)
            steps.append((row, inv_row, mult))
        inv[b] = inv_head
        for i in range(b + 1, groups):
            for row, inv_row, mult in steps:
                rows[i] = rows[i] - mult[i - b] * row
                inv[i] = inv[i] - mult[i - b] * inv_row
    return inv


def update_kernel(block_ref, rows_ref, cols_ref, tile_ref, panel_ref, mine_ref, given_ref, first_ref, second_ref):
    def factor_into(block, out_ref):
        inv = inverse_factor([block[SUB * g : SUB * g + SUB] for g in range(PW // SUB)])
        for g, rows in enumerate(inv):
            out_ref[SUB * g : SUB * g + SUB, :] = rows

    factor_into(block_ref[:PW, :PW], first_ref)
    corner = dot_t(block_ref[PW:, :PW], first_ref[...])
    factor_into(block_ref[PW:, PW:] - dot_t(corner, corner), second_ref)

    first, second, below = in_two(first_ref[...]), in_two(second_ref[...]), in_two(corner)

    def panels_of(ref):
        left = split_dot_t(in_two(ref[:, :PW]), first)
        left_two = in_two(left)
        right = split_dot_t(in_two(ref[:, PW:] - split_dot_t(left_two, below)), second)
        return left, right, left_two, in_two(right)

    row_left, row_right, row_left_two, row_right_two = panels_of(rows_ref)
    _, _, col_left_two, col_right_two = panels_of(cols_ref)
    kept = panel_ref.shape[0]
    panel_ref[:, :PW] = row_left[:kept]
    panel_ref[:, PW:] = row_right[:kept]

    def rows_of(two, part):
        return two[0][part], two[1][part]

    for out_ref, start in ((given_ref, kept), (mine_ref, 0)):
        part = slice(start, start + kept)
        out_ref[...] = (
            tile_ref[part, :]
            - split_dot_t(rows_of(row_left_two, part), col_left_two)
            - split_dot_t(rows_of(row_right_two, part), col_right_two)
        )


def updated(block, rows, cols, tile):
    kept = rows.shape[0] // 2
    wide = jax.ShapeDtypeStruct((kept, tile.shape[1]), jnp.float32)
    return pl.pallas_call(
        update_kernel,
        out_shape=(jax.ShapeDtypeStruct((kept, 2 * PW), jnp.float32), wide, wide),
        scratch_shapes=[pltpu.VMEM((PW, PW), jnp.float32)] * 2,
        cost_estimate=pl.CostEstimate(flops=400_000_000, bytes_accessed=4_000_000, transcendentals=256),
    )(block, rows, cols, tile)


def per_device(points, landmark_index, targets, ridge_shift):
    rows_here = landmark_index.shape[0]
    block_points = points.shape[0]
    row_pos = lax.axis_index(ROWS)
    col_pos = lax.axis_index("cols")
    y_pos = lax.axis_index(Y)
    n_rows = lax.axis_size(ROWS)
    n_y = lax.axis_size(Y)
    per_y = n_rows // n_y
    quarter = C // 2 // n_rows
    half = C // 4
    half_pos = lax.axis_index("half")
    upper = half_pos == 1
    ridge = ridge_shift[0]
    across = [(y, n_y - 1 - y) for y in range(n_y)]
    swap = [(0, 1), (1, 0)]

    def ordered(flag, mine, other, axis):
        return jnp.concatenate([jnp.where(flag, other, mine), jnp.where(flag, mine, other)], axis=axis)

    local_index = landmark_index - row_pos * block_points
    embedded = points.at[local_index].get(mode="promise_in_bounds")
    own = lax.dynamic_slice_in_dim(embedded, col_pos * quarter, quarter, 0)
    peer_embedded = lax.ppermute(embedded, Y, across)
    own_line = to_all(own, "z")
    column_emb = lax.optimization_barrier(to_all(own_line, NEAR).reshape(half, -1))
    own_targets = jnp.concatenate([targets, lax.ppermute(targets, Y, across)], axis=0)
    peer_targets = lax.ppermute(own_targets, "cols", swap)
    pair_targets = lax.optimization_barrier(ordered(col_pos == 1, own_targets, peer_targets, 1))
    rows_emb = lax.optimization_barrier(jnp.concatenate([embedded, peer_embedded], axis=0))

    rows_sq = squares(rows_emb)
    col_sq = squares(column_emb)
    peer_pos = row_pos + (n_y - 1 - 2 * y_pos) * per_y
    local = lax.iota(jnp.int32, rows_here)
    row_place = jnp.concatenate([row_pos * rows_here + local, peer_pos * rows_here + local])
    column = half_pos * half + lax.iota(jnp.int32, half)
    col_place = column // quarter * rows_here + col_pos * quarter + column % quarter

    tile = gaussian(rows_emb, rows_sq, column_emb, col_sq)
    tile = tile + jnp.where(row_place[:, None] == col_place[None, :], ridge, 0.0)
    partial = lax.dot_general(
        pair_targets, tile, (((0,), (0,)), ((), ())), precision=lax.Precision.HIGH, preferred_element_type=jnp.float32
    )
    n_plane = lax.axis_size(PLANE)
    n_z = lax.axis_size("z")
    arrived = lax.all_to_all(partial.reshape(n_plane, -1, half), PLANE, 0, 0, tiled=True)
    nearer = arrived.reshape(2, n_plane // 2, -1, half).sum(axis=1)
    nearer = nearer.reshape(2, n_z, -1, half).swapaxes(0, 1)
    projected = lax.all_to_all(nearer, "z", 0, 0, tiled=True).sum(axis=0)
    projected = jnp.concatenate([projected[0], projected[1]], axis=1)

    sent_heads = lax.ppermute(column_emb[:PW], Y, [(y, n_y - 1 - y) for y in range(n_y // 2)])
    own_heads = jnp.where(upper, sent_heads, column_emb[:PW])
    heads = ordered(col_pos == 1, own_heads, lax.ppermute(own_heads, "cols", swap), 0)
    heads_sq = squares(heads)
    head = lax.iota(jnp.int32, 2 * PW)
    head_place = head % PW // quarter * rows_here + head // PW * quarter + head % quarter

    def at_heads(emb, emb_sq, place):
        base = gaussian(emb, emb_sq, heads, heads_sq)
        return base + jnp.where(place[:, None] == head_place[None, :], ridge, 0.0)

    operands = (
        at_heads(heads, heads_sq, head_place),
        at_heads(rows_emb, rows_sq, row_place),
        at_heads(column_emb, col_sq, col_place),
        tile,
    )
    panels, mine, given = updated(*operands)
    taken = lax.ppermute(given, Y, across)
    remainder = jnp.concatenate(
        [jnp.where(upper, taken, mine)[:, PW:], jnp.where(upper, mine, taken)], axis=1
    )
    return projected, panels, remainder


def solution(mesh):
    split = Mesh(
        mesh.devices.reshape(2, 2, 4, 8, mesh.shape["cols"]), ("half", "near", "x", "z", "cols")
    )
    placed = (P(ROWS, None), P(ROWS), P(ROWS, "cols"), P())
    return jax.shard_map(
        per_device,
        mesh=split,
        in_specs=placed,
        out_specs=(P(ROWS, "cols"), P(ROWS, None), P(ROWS, "cols")),
        check_vma=False,
    )
```

```python
import jax
import jax.numpy as jnp
from jax import lax
from jax.experimental import pallas as pl
from jax.experimental.pallas import tpu as pltpu
from jax.sharding import Mesh
from jax.sharding import PartitionSpec as P


C = 2048
PW = 128
Y = ("half", "near")
PLANE = ("half", "near", "x")
NEAR = ("near", "x")
ROWS = ("half", "near", "x", "z")
SUB = 8
CHUNK = 128

exact_mode = lax.Precision.HIGHEST


def to_all(x, axis):
    peers = lax.axis_size(axis)
    return lax.all_to_all(jnp.broadcast_to(x[None], (peers, *x.shape)), axis, 0, 0, tiled=True)


def dot_t(left, right):
    return lax.dot_general(
        left, right, (((1,), (1,)), ((), ())), precision=exact_mode, preferred_element_type=jnp.float32
    )


def in_two(x):
    high = x.astype(jnp.bfloat16)
    return high, (x - high.astype(jnp.float32)).astype(jnp.bfloat16)


def split_dot_t(left, right):
    def part(a, b):
        return lax.dot_general(a, b, (((1,), (1,)), ((), ())), preferred_element_type=jnp.float32)

    return part(left[0], right[1]) + part(left[1], right[0]) + part(left[0], right[0])


def gaussian(left, left_sq, right, right_sq):
    cross = dot_t(left, right)
    return jnp.exp(-(left_sq[:, None] + right_sq[None, :] - 2.0 * cross) / (2.0 * left.shape[1]))


def squares(x):
    return jnp.sum(x * x, axis=1)


def inverse_factor(rows, between):
    groups = len(rows)
    ids = lax.broadcasted_iota(jnp.int32, (SUB, PW), 0)
    lanes = lax.broadcasted_iota(jnp.int32, (SUB, PW), 1)
    inv = [jnp.where(lanes == ids + SUB * g, 1.0, 0.0).astype(jnp.float32) for g in range(groups)]
    for b in range(groups):
        cols = [
            [jnp.broadcast_to(rows[i][:, SUB * b + j : SUB * b + j + 1], (SUB, PW)) for i in range(b, groups)]
            for j in range(SUB)
        ]
        head, inv_head = rows[b], inv[b]
        steps = []
        for k in range(SUB):
            spread = [jnp.broadcast_to(cols[k][0][j : j + 1], (SUB, PW)) for j in range(k, SUB)]
            scale = lax.rsqrt(spread[0])
            row = jnp.broadcast_to(head[k : k + 1], (SUB, PW)) * scale
            inv_row = jnp.broadcast_to(inv_head[k : k + 1], (SUB, PW)) * scale
            mult = [c * scale for c in cols[k]]
            mult[0] = jnp.where(ids > k, mult[0], 0.0)
            for j in range(k + 1, SUB):
                there = spread[j - k] * scale
                cols[j] = [c - m * there for c, m in zip(cols[j], mult)]
            head = head - mult[0] * row
            inv_head = jnp.where(ids == k, inv_row, inv_head - mult[0] * inv_row)
            steps.append((row, inv_row, mult))
        inv[b] = inv_head
        for i in range(b + 1, groups):
            for row, inv_row, mult in steps:
                rows[i] = rows[i] - mult[i - b] * row
                inv[i] = inv[i] - mult[i - b] * inv_row
        between(b)
    return inv


def in_three(x):
    high, rest = x.astype(jnp.bfloat16), x
    rest = rest - high.astype(jnp.float32)
    middle = rest.astype(jnp.bfloat16)
    return high, middle, (rest - middle.astype(jnp.float32)).astype(jnp.bfloat16)


def full_dot_t(left, right):
    total = None
    for i, j in ((2, 0), (0, 2), (1, 1), (1, 0), (0, 1), (0, 0)):
        part = lax.dot_general(
            left[i], right[j], (((1,), (1,)), ((), ())), preferred_element_type=jnp.float32
        )
        total = part if total is None else total + part
    return total


def update_kernel(
    place_ref, ridge_ref, block_ref, heads_ref, head_sq_ref, rows_emb_ref, cols_emb_ref, tile_ref,
    panel_ref, mine_ref, given_ref, first_ref, second_ref, rows_ref, cols_ref,
):
    heads = in_three(heads_ref[...])
    head_sq = head_sq_ref[...]
    n_heads, width = heads_ref.shape
    kept = panel_ref.shape[0]
    head = lax.broadcasted_iota(jnp.int32, (CHUNK, n_heads), 1)
    head_place = (head % PW >> 3) * kept + (head // PW) * SUB + (head & (SUB - 1))
    local = lax.broadcasted_iota(jnp.int32, (CHUNK, n_heads), 0)

    def chunk(step):
        emb_ref, out_ref, start = (
            (rows_emb_ref, rows_ref, step * CHUNK)
            if step < rows_ref.shape[0] // CHUNK
            else (cols_emb_ref, cols_ref, step * CHUNK - rows_ref.shape[0])
        )
        emb = emb_ref[start : start + CHUNK, :]
        if emb_ref is rows_emb_ref:
            place = place_ref[start // kept] + start % kept + local
        else:
            column = place_ref[2] + start + local
            place = (column >> 3) * kept + place_ref[3] + (column & (SUB - 1))
        cross = full_dot_t(in_three(emb), heads)
        square = jnp.sum(emb * emb, axis=1, keepdims=True)
        base = jnp.exp(-(square + head_sq - 2.0 * cross) / (2.0 * width))
        out_ref[start : start + CHUNK, :] = base + jnp.where(place == head_place, ridge_ref[0], 0.0)

    chunks = (rows_ref.shape[0] + cols_ref.shape[0]) // CHUNK
    groups = PW // SUB

    def between(panel):
        def run(b):
            done = panel * groups + b
            for step in range(done * chunks // (2 * groups), (done + 1) * chunks // (2 * groups)):
                chunk(step)

        return run

    def factor_into(block, out_ref, run):
        inv = inverse_factor([block[SUB * g : SUB * g + SUB] for g in range(groups)], run)
        for g, rows in enumerate(inv):
            out_ref[SUB * g : SUB * g + SUB, :] = rows

    factor_into(block_ref[:PW, :PW], first_ref, between(0))
    corner = dot_t(block_ref[PW:, :PW], first_ref[...])
    factor_into(block_ref[PW:, PW:] - dot_t(corner, corner), second_ref, between(1))

    first, second, below = in_two(first_ref[...]), in_two(second_ref[...]), in_two(corner)

    def panels_of(ref):
        left = split_dot_t(in_two(ref[:, :PW]), first)
        left_two = in_two(left)
        right = split_dot_t(in_two(ref[:, PW:] - split_dot_t(left_two, below)), second)
        return left, right, left_two, in_two(right)

    row_left, row_right, row_left_two, row_right_two = panels_of(rows_ref)
    _, _, col_left_two, col_right_two = panels_of(cols_ref)
    panel_ref[:, :PW] = row_left[:kept]
    panel_ref[:, PW:] = row_right[:kept]

    def rows_of(two, part):
        return two[0][part], two[1][part]

    for out_ref, start in ((given_ref, kept), (mine_ref, 0)):
        part = slice(start, start + kept)
        out_ref[...] = (
            tile_ref[part, :]
            - split_dot_t(rows_of(row_left_two, part), col_left_two)
            - split_dot_t(rows_of(row_right_two, part), col_right_two)
        )


def updated(place, ridge, block, heads, head_sq, rows_emb, cols_emb, tile):
    kept = rows_emb.shape[0] // 2
    wide = jax.ShapeDtypeStruct((kept, tile.shape[1]), jnp.float32)
    scalar = pl.BlockSpec(memory_space=pltpu.SMEM)
    return pl.pallas_call(
        update_kernel,
        out_shape=(jax.ShapeDtypeStruct((kept, 2 * PW), jnp.float32), wide, wide),
        in_specs=[scalar, scalar] + [pl.BlockSpec(memory_space=pltpu.VMEM)] * 6,
        scratch_shapes=[pltpu.VMEM((PW, PW), jnp.float32)] * 2
        + [pltpu.VMEM((emb.shape[0], 2 * PW), jnp.float32) for emb in (rows_emb, cols_emb)],
        cost_estimate=pl.CostEstimate(flops=900_000_000, bytes_accessed=8_000_000, transcendentals=256),
    )(place, ridge, block, heads, head_sq, rows_emb, cols_emb, tile)


def per_device(points, landmark_index, targets, ridge_shift):
    rows_here = landmark_index.shape[0]
    block_points = points.shape[0]
    row_pos = lax.axis_index(ROWS)
    col_pos = lax.axis_index("cols")
    y_pos = lax.axis_index(Y)
    n_rows = lax.axis_size(ROWS)
    n_y = lax.axis_size(Y)
    per_y = n_rows // n_y
    quarter = C // 2 // n_rows
    half = C // 4
    half_pos = lax.axis_index("half")
    upper = half_pos == 1
    ridge = ridge_shift[0]
    across = [(y, n_y - 1 - y) for y in range(n_y)]
    swap = [(0, 1), (1, 0)]

    def ordered(flag, mine, other, axis):
        return jnp.concatenate([jnp.where(flag, other, mine), jnp.where(flag, mine, other)], axis=axis)

    local_index = landmark_index - row_pos * block_points
    embedded = points.at[local_index].get(mode="promise_in_bounds")
    own = lax.dynamic_slice_in_dim(embedded, col_pos * quarter, quarter, 0)
    peer_embedded = lax.ppermute(embedded, Y, across)
    own_line = to_all(own, "z")
    column_emb = lax.optimization_barrier(to_all(own_line, NEAR).reshape(half, -1))
    own_targets = jnp.concatenate([targets, lax.ppermute(targets, Y, across)], axis=0)
    peer_targets = lax.ppermute(own_targets, "cols", swap)
    pair_targets = lax.optimization_barrier(ordered(col_pos == 1, own_targets, peer_targets, 1))
    rows_emb = lax.optimization_barrier(jnp.concatenate([embedded, peer_embedded], axis=0))

    rows_sq = squares(rows_emb)
    col_sq = squares(column_emb)
    peer_pos = row_pos + (n_y - 1 - 2 * y_pos) * per_y
    local = lax.iota(jnp.int32, rows_here)
    row_place = jnp.concatenate([row_pos * rows_here + local, peer_pos * rows_here + local])
    column = half_pos * half + lax.iota(jnp.int32, half)
    col_place = column // quarter * rows_here + col_pos * quarter + column % quarter

    tile = gaussian(rows_emb, rows_sq, column_emb, col_sq)
    tile = lax.optimization_barrier(
        tile + jnp.where(row_place[:, None] == col_place[None, :], ridge, 0.0)
    )
    partial = lax.dot_general(
        pair_targets, tile, (((0,), (0,)), ((), ())), precision=lax.Precision.HIGH, preferred_element_type=jnp.float32
    )
    n_plane = lax.axis_size(PLANE)
    n_z = lax.axis_size("z")
    arrived = lax.all_to_all(partial.reshape(n_plane, -1, half), PLANE, 0, 0, tiled=True)
    nearer = arrived.reshape(2, n_plane // 2, -1, half).sum(axis=1)
    nearer = nearer.reshape(2, n_z, -1, half).swapaxes(0, 1)
    projected = lax.all_to_all(nearer, "z", 0, 0, tiled=True).sum(axis=0)
    projected = jnp.concatenate([projected[0], projected[1]], axis=1)

    sent_heads = lax.ppermute(column_emb[:PW], Y, [(y, n_y - 1 - y) for y in range(n_y // 2)])
    own_heads = jnp.where(upper, sent_heads, column_emb[:PW])
    heads = ordered(col_pos == 1, own_heads, lax.ppermute(own_heads, "cols", swap), 0)
    heads_sq = squares(heads)
    head = lax.iota(jnp.int32, 2 * PW)
    head_place = head % PW // quarter * rows_here + head // PW * quarter + head % quarter

    def at_heads(emb, emb_sq, place):
        base = gaussian(emb, emb_sq, heads, heads_sq)
        return base + jnp.where(place[:, None] == head_place[None, :], ridge, 0.0)

    places = jnp.stack(
        [row_pos * rows_here, peer_pos * rows_here, half_pos * half, col_pos * quarter]
    ).astype(jnp.int32)
    operands = (
        places,
        ridge_shift,
        at_heads(heads, heads_sq, head_place),
        heads,
        heads_sq[None, :],
        rows_emb,
        column_emb,
        tile,
    )
    panels, mine, given = updated(*operands)
    taken = lax.ppermute(given, Y, across)
    remainder = jnp.concatenate(
        [jnp.where(upper, taken, mine)[:, PW:], jnp.where(upper, mine, taken)], axis=1
    )
    return projected, panels, remainder


def solution(mesh):
    split = Mesh(
        mesh.devices.reshape(2, 2, 4, 8, mesh.shape["cols"]), ("half", "near", "x", "z", "cols")
    )
    placed = (P(ROWS, None), P(ROWS), P(ROWS, "cols"), P())
    return jax.shard_map(
        per_device,
        mesh=split,
        in_specs=placed,
        out_specs=(P(ROWS, "cols"), P(ROWS, None), P(ROWS, "cols")),
        check_vma=False,
    )
```

```python
import jax
import jax.numpy as jnp
from jax import lax
from jax.experimental import pallas as pl
from jax.experimental.pallas import tpu as pltpu
from jax.sharding import Mesh
from jax.sharding import PartitionSpec as P


C = 2048
PW = 128
Y = ("half", "near")
PLANE = ("half", "near", "x")
NEAR = ("near", "x")
ROWS = ("half", "near", "x", "z")
SUB = 8
CHUNK = 128

exact_mode = lax.Precision.HIGHEST


def to_all(x, axis):
    peers = lax.axis_size(axis)
    return lax.all_to_all(jnp.broadcast_to(x[None], (peers, *x.shape)), axis, 0, 0, tiled=True)


def dot_t(left, right):
    return lax.dot_general(
        left, right, (((1,), (1,)), ((), ())), precision=exact_mode, preferred_element_type=jnp.float32
    )


def in_two(x):
    high = x.astype(jnp.bfloat16)
    return high, (x - high.astype(jnp.float32)).astype(jnp.bfloat16)


def split_dot_t(left, right):
    def part(a, b):
        return lax.dot_general(a, b, (((1,), (1,)), ((), ())), preferred_element_type=jnp.float32)

    return part(left[0], right[1]) + part(left[1], right[0]) + part(left[0], right[0])


def gaussian(left, left_sq, right, right_sq):
    cross = dot_t(left, right)
    return jnp.exp(-(left_sq[:, None] + right_sq[None, :] - 2.0 * cross) / (2.0 * left.shape[1]))


def squares(x):
    return jnp.sum(x * x, axis=1)


def inverse_factor(rows, between):
    groups = len(rows)
    ids = lax.broadcasted_iota(jnp.int32, (SUB, PW), 0)
    lanes = lax.broadcasted_iota(jnp.int32, (SUB, PW), 1)
    inv = [jnp.where(lanes == ids + SUB * g, 1.0, 0.0).astype(jnp.float32) for g in range(groups)]
    for b in range(groups):
        cols = [
            [jnp.broadcast_to(rows[i][:, SUB * b + j : SUB * b + j + 1], (SUB, PW)) for i in range(b, groups)]
            for j in range(SUB)
        ]
        head, inv_head = rows[b], inv[b]
        steps = []
        for k in range(SUB):
            spread = [jnp.broadcast_to(cols[k][0][j : j + 1], (SUB, PW)) for j in range(k, SUB)]
            scale = lax.rsqrt(spread[0])
            row = jnp.broadcast_to(head[k : k + 1], (SUB, PW)) * scale
            inv_row = jnp.broadcast_to(inv_head[k : k + 1], (SUB, PW)) * scale
            mult = [c * scale for c in cols[k]]
            mult[0] = jnp.where(ids > k, mult[0], 0.0)
            for j in range(k + 1, SUB):
                there = spread[j - k] * scale
                cols[j] = [c - m * there for c, m in zip(cols[j], mult)]
            head = head - mult[0] * row
            inv_head = jnp.where(ids == k, inv_row, inv_head - mult[0] * inv_row)
            steps.append((row, inv_row, mult))
        inv[b] = inv_head
        for i in range(b + 1, groups):
            for row, inv_row, mult in steps:
                rows[i] = rows[i] - mult[i - b] * row
                inv[i] = inv[i] - mult[i - b] * inv_row
        between(b)
    return inv


def in_three(x):
    high, rest = x.astype(jnp.bfloat16), x
    rest = rest - high.astype(jnp.float32)
    middle = rest.astype(jnp.bfloat16)
    return high, middle, (rest - middle.astype(jnp.float32)).astype(jnp.bfloat16)


def full_dot_t(left, right):
    total = None
    for i, j in ((2, 0), (0, 2), (1, 1), (1, 0), (0, 1), (0, 0)):
        part = lax.dot_general(
            left[i], right[j], (((1,), (1,)), ((), ())), preferred_element_type=jnp.float32
        )
        total = part if total is None else total + part
    return total


def update_kernel(
    place_ref, ridge_ref, head_0_ref, head_1_ref, rows_emb_ref, cols_emb_ref, tile_ref,
    panel_ref, mine_ref, given_ref, first_ref, second_ref, rows_ref, cols_ref,
):
    head_emb = jnp.concatenate([head_0_ref[...], head_1_ref[...]], axis=0)
    heads = in_three(head_emb)
    n_heads, width = head_emb.shape
    ones = jnp.ones((SUB, width), jnp.bfloat16)
    head_sq = sum(
        lax.dot_general(ones, part, (((1,), (1,)), ((), ())), preferred_element_type=jnp.float32)
        for part in reversed(in_three(head_emb * head_emb))
    )[:1]

    def distances(emb, parts):
        square = jnp.sum(emb * emb, axis=1, keepdims=True)
        return jnp.exp(-(square + head_sq - 2.0 * full_dot_t(parts, heads)) / (2.0 * width))

    same = lax.broadcasted_iota(jnp.int32, (n_heads, n_heads), 0) == lax.broadcasted_iota(
        jnp.int32, (n_heads, n_heads), 1
    )
    block = distances(head_emb, heads) + jnp.where(same, ridge_ref[0], 0.0)
    kept = panel_ref.shape[0]
    head = lax.broadcasted_iota(jnp.int32, (CHUNK, n_heads), 1)
    head_place = (head % PW >> 3) * kept + (head // PW) * SUB + (head & (SUB - 1))
    local = lax.broadcasted_iota(jnp.int32, (CHUNK, n_heads), 0)

    def chunk(step):
        emb_ref, out_ref, start = (
            (rows_emb_ref, rows_ref, step * CHUNK)
            if step < rows_ref.shape[0] // CHUNK
            else (cols_emb_ref, cols_ref, step * CHUNK - rows_ref.shape[0])
        )
        emb = emb_ref[start : start + CHUNK, :]
        if emb_ref is rows_emb_ref:
            place = place_ref[start // kept] + start % kept + local
        else:
            column = place_ref[2] + start + local
            place = (column >> 3) * kept + place_ref[3] + (column & (SUB - 1))
        base = distances(emb, in_three(emb))
        out_ref[start : start + CHUNK, :] = base + jnp.where(place == head_place, ridge_ref[0], 0.0)

    chunks = (rows_ref.shape[0] + cols_ref.shape[0]) // CHUNK
    groups = PW // SUB

    def between(panel):
        def run(b):
            done = panel * groups + b
            for step in range(done * chunks // (2 * groups), (done + 1) * chunks // (2 * groups)):
                chunk(step)

        return run

    def factor_into(block, out_ref, run):
        inv = inverse_factor([block[SUB * g : SUB * g + SUB] for g in range(groups)], run)
        for g, rows in enumerate(inv):
            out_ref[SUB * g : SUB * g + SUB, :] = rows

    factor_into(block[:PW, :PW], first_ref, between(0))
    corner = dot_t(block[PW:, :PW], first_ref[...])
    factor_into(block[PW:, PW:] - dot_t(corner, corner), second_ref, between(1))

    first, second, below = in_two(first_ref[...]), in_two(second_ref[...]), in_two(corner)

    def panels_of(ref):
        left = split_dot_t(in_two(ref[:, :PW]), first)
        left_two = in_two(left)
        right = split_dot_t(in_two(ref[:, PW:] - split_dot_t(left_two, below)), second)
        return left, right, left_two, in_two(right)

    row_left, row_right, row_left_two, row_right_two = panels_of(rows_ref)
    _, _, col_left_two, col_right_two = panels_of(cols_ref)
    panel_ref[:, :PW] = row_left[:kept]
    panel_ref[:, PW:] = row_right[:kept]

    def rows_of(two, part):
        return two[0][part], two[1][part]

    for out_ref, start in ((given_ref, kept), (mine_ref, 0)):
        part = slice(start, start + kept)
        out_ref[...] = (
            tile_ref[part, :]
            - split_dot_t(rows_of(row_left_two, part), col_left_two)
            - split_dot_t(rows_of(row_right_two, part), col_right_two)
        )


def updated(place, ridge, head_0, head_1, rows_emb, cols_emb, tile):
    kept = rows_emb.shape[0] // 2
    wide = jax.ShapeDtypeStruct((kept, tile.shape[1]), jnp.float32)
    scalar = pl.BlockSpec(memory_space=pltpu.SMEM)
    return pl.pallas_call(
        update_kernel,
        out_shape=(jax.ShapeDtypeStruct((kept, 2 * PW), jnp.float32), wide, wide),
        in_specs=[scalar, scalar] + [pl.BlockSpec(memory_space=pltpu.VMEM)] * 5,
        scratch_shapes=[pltpu.VMEM((PW, PW), jnp.float32)] * 2
        + [pltpu.VMEM((emb.shape[0], 2 * PW), jnp.float32) for emb in (rows_emb, cols_emb)],
        cost_estimate=pl.CostEstimate(flops=900_000_000, bytes_accessed=8_000_000, transcendentals=256),
    )(place, ridge, head_0, head_1, rows_emb, cols_emb, tile)


def take_kernel(start_ref, index_ref, points_ref, emb_ref, own_ref):
    point = lax.broadcasted_iota(jnp.int32, (points_ref.shape[0], index_ref.shape[1]), 0)
    hot = jnp.where(point == index_ref[...] - start_ref[0], 1.0, 0.0).astype(jnp.bfloat16)
    high, middle, low = (
        lax.dot_general(hot, part, (((0,), (0,)), ((), ())), preferred_element_type=jnp.float32)
        for part in in_three(points_ref[...])
    )
    emb_ref[...] = high + middle + low
    own = emb_ref[pl.ds(pl.multiple_of(start_ref[1], SUB), SUB), :]
    for peer in range(own_ref.shape[0]):
        own_ref[peer] = own


def taken_rows(start, index, points, peers):
    width = points.shape[1]
    vmem = pl.BlockSpec(memory_space=pltpu.VMEM)
    return pl.pallas_call(
        take_kernel,
        out_shape=(
            jax.ShapeDtypeStruct((index.shape[0], width), jnp.float32),
            jax.ShapeDtypeStruct((peers, SUB, width), jnp.float32),
        ),
        in_specs=[pl.BlockSpec(memory_space=pltpu.SMEM), vmem, vmem],
        compiler_params=pltpu.CompilerParams(vmem_limit_bytes=20 * 2**20),
        cost_estimate=pl.CostEstimate(flops=600_000_000, bytes_accessed=3_000_000, transcendentals=0),
    )(start, index[None, :], points)


def chosen(*values):
    slots = lax.iota(jnp.int32, len(values))
    table = jnp.zeros(len(values), jnp.int32)
    for slot, value in enumerate(values):
        table = jnp.where(slots == slot, value, table)
    return table


def per_device(points, landmark_index, targets, ridge_shift):
    rows_here = landmark_index.shape[0]
    block_points = points.shape[0]
    row_pos = lax.axis_index(ROWS)
    col_pos = lax.axis_index("cols")
    y_pos = lax.axis_index(Y)
    n_rows = lax.axis_size(ROWS)
    n_y = lax.axis_size(Y)
    per_y = n_rows // n_y
    quarter = C // 2 // n_rows
    half = C // 4
    half_pos = lax.axis_index("half")
    upper = half_pos == 1
    ridge = ridge_shift[0]
    across = [(y, n_y - 1 - y) for y in range(n_y)]
    swap = [(0, 1), (1, 0)]

    def ordered(flag, mine, other, axis):
        return jnp.concatenate([jnp.where(flag, other, mine), jnp.where(flag, mine, other)], axis=axis)

    n_z = lax.axis_size("z")
    start = chosen(row_pos * block_points, col_pos * quarter, half_pos * half)
    embedded, own_copies = taken_rows(start, landmark_index, points, n_z)
    peer_embedded = lax.ppermute(embedded, Y, across)
    own_line = lax.all_to_all(own_copies, "z", 0, 0, tiled=True)
    column_emb = lax.optimization_barrier(to_all(own_line, NEAR).reshape(half, -1))
    own_targets = jnp.concatenate([targets, lax.ppermute(targets, Y, across)], axis=0)
    peer_targets = lax.ppermute(own_targets, "cols", swap)
    pair_targets = lax.optimization_barrier(ordered(col_pos == 1, own_targets, peer_targets, 1))
    peer_pos = row_pos + (n_y - 1 - 2 * y_pos) * per_y
    places = chosen(row_pos * rows_here, peer_pos * rows_here, half_pos * half, col_pos * quarter)
    rows_emb, places = lax.optimization_barrier(
        (jnp.concatenate([embedded, peer_embedded], axis=0), places)
    )

    rows_sq = squares(rows_emb)
    col_sq = squares(column_emb)
    local = lax.iota(jnp.int32, rows_here)
    row_place = jnp.concatenate([row_pos * rows_here + local, peer_pos * rows_here + local])
    column = half_pos * half + lax.iota(jnp.int32, half)
    col_place = column // quarter * rows_here + col_pos * quarter + column % quarter

    tile = gaussian(rows_emb, rows_sq, column_emb, col_sq)
    tile = lax.optimization_barrier(
        tile + jnp.where(row_place[:, None] == col_place[None, :], ridge, 0.0)
    )
    partial = lax.dot_general(
        pair_targets, tile, (((0,), (0,)), ((), ())), precision=lax.Precision.HIGH, preferred_element_type=jnp.float32
    )
    n_plane = lax.axis_size(PLANE)
    arrived = lax.all_to_all(partial.reshape(n_plane, -1, half), PLANE, 0, 0, tiled=True)
    nearer = arrived.reshape(2, n_plane // 2, -1, half).sum(axis=1)
    nearer = nearer.reshape(2, n_z, -1, half).swapaxes(0, 1)
    projected = lax.all_to_all(nearer, "z", 0, 0, tiled=True).sum(axis=0)
    projected = jnp.concatenate([projected[0], projected[1]], axis=1)

    sent_heads = lax.ppermute(column_emb[:PW], Y, [(y, n_y - 1 - y) for y in range(n_y // 2)])
    own_heads = jnp.where(upper, sent_heads, column_emb[:PW])
    peer_heads = lax.ppermute(own_heads, "cols", swap)
    swapped = col_pos == 1
    head_0 = jnp.where(swapped, peer_heads, own_heads)
    head_1 = jnp.where(swapped, own_heads, peer_heads)

    panels, mine, given = updated(
        places, ridge_shift, head_0, head_1, rows_emb, column_emb, tile
    )
    taken = lax.ppermute(given, Y, across)
    remainder = jnp.concatenate(
        [jnp.where(upper, taken, mine)[:, PW:], jnp.where(upper, mine, taken)], axis=1
    )
    return projected, panels, remainder


def solution(mesh):
    split = Mesh(
        mesh.devices.reshape(2, 2, 4, 8, mesh.shape["cols"]), ("half", "near", "x", "z", "cols")
    )
    placed = (P(ROWS, None), P(ROWS), P(ROWS, "cols"), P())
    return jax.shard_map(
        per_device,
        mesh=split,
        in_specs=placed,
        out_specs=(P(ROWS, "cols"), P(ROWS, None), P(ROWS, "cols")),
        check_vma=False,
    )
```

```python
import jax
import jax.numpy as jnp
from jax import lax
from jax.experimental import pallas as pl
from jax.experimental.pallas import tpu as pltpu
from jax.sharding import Mesh
from jax.sharding import PartitionSpec as P


C = 2048
PW = 128
Y = ("half", "near")
PLANE = ("half", "near", "x")
NEAR = ("near", "x")
ROWS = ("half", "near", "x", "z")
SUB = 8
CHUNK = 128

exact_mode = lax.Precision.HIGHEST


def to_all(x, axis):
    peers = lax.axis_size(axis)
    return lax.all_to_all(jnp.broadcast_to(x[None], (peers, *x.shape)), axis, 0, 0, tiled=True)


def dot_t(left, right):
    return lax.dot_general(
        left, right, (((1,), (1,)), ((), ())), precision=exact_mode, preferred_element_type=jnp.float32
    )


def in_two(x):
    high = x.astype(jnp.bfloat16)
    return high, (x - high.astype(jnp.float32)).astype(jnp.bfloat16)


def split_dot_t(left, right):
    def part(a, b):
        return lax.dot_general(a, b, (((1,), (1,)), ((), ())), preferred_element_type=jnp.float32)

    return part(left[0], right[1]) + part(left[1], right[0]) + part(left[0], right[0])


def gaussian(left, left_sq, right, right_sq):
    cross = dot_t(left, right)
    return jnp.exp(-(left_sq[:, None] + right_sq[None, :] - 2.0 * cross) / (2.0 * left.shape[1]))


def squares(x):
    return jnp.sum(x * x, axis=1)


def inverse_factor(rows, between):
    groups = len(rows)
    ids = lax.broadcasted_iota(jnp.int32, (SUB, PW), 0)
    lanes = lax.broadcasted_iota(jnp.int32, (SUB, PW), 1)
    inv = [jnp.where(lanes == ids + SUB * g, 1.0, 0.0).astype(jnp.float32) for g in range(groups)]
    for b in range(groups):
        cols = [
            [jnp.broadcast_to(rows[i][:, SUB * b + j : SUB * b + j + 1], (SUB, PW)) for i in range(b, groups)]
            for j in range(SUB)
        ]
        head, inv_head = rows[b], inv[b]
        steps = []
        for k in range(SUB):
            spread = [jnp.broadcast_to(cols[k][0][j : j + 1], (SUB, PW)) for j in range(k, SUB)]
            scale = lax.rsqrt(spread[0])
            row = jnp.broadcast_to(head[k : k + 1], (SUB, PW)) * scale
            inv_row = jnp.broadcast_to(inv_head[k : k + 1], (SUB, PW)) * scale
            mult = [c * scale for c in cols[k]]
            mult[0] = jnp.where(ids > k, mult[0], 0.0)
            for j in range(k + 1, SUB):
                there = spread[j - k] * scale
                cols[j] = [c - m * there for c, m in zip(cols[j], mult)]
            head = head - mult[0] * row
            inv_head = jnp.where(ids == k, inv_row, inv_head - mult[0] * inv_row)
            steps.append((row, inv_row, mult))
        inv[b] = inv_head
        for i in range(b + 1, groups):
            for row, inv_row, mult in steps:
                rows[i] = rows[i] - mult[i - b] * row
                inv[i] = inv[i] - mult[i - b] * inv_row
        between(b)
    return inv


def in_three(x):
    high, rest = x.astype(jnp.bfloat16), x
    rest = rest - high.astype(jnp.float32)
    middle = rest.astype(jnp.bfloat16)
    return high, middle, (rest - middle.astype(jnp.float32)).astype(jnp.bfloat16)


def full_dot_t(left, right):
    total = None
    for i, j in ((2, 0), (0, 2), (1, 1), (1, 0), (0, 1), (0, 0)):
        part = lax.dot_general(
            left[i], right[j], (((1,), (1,)), ((), ())), preferred_element_type=jnp.float32
        )
        total = part if total is None else total + part
    return total


def update_kernel(
    place_ref, ridge_ref, head_0_ref, head_1_ref, rows_emb_ref, cols_emb_ref, tile_ref,
    panel_ref, mine_ref, given_ref, first_ref, second_ref, rows_ref, cols_ref,
):
    head_emb = jnp.concatenate([head_0_ref[...], head_1_ref[...]], axis=0)
    heads = in_three(head_emb)
    n_heads, width = head_emb.shape
    ones = jnp.ones((SUB, width), jnp.bfloat16)
    head_sq = sum(
        lax.dot_general(ones, part, (((1,), (1,)), ((), ())), preferred_element_type=jnp.float32)
        for part in reversed(in_three(head_emb * head_emb))
    )[:1]

    def distances(emb, parts):
        square = jnp.sum(emb * emb, axis=1, keepdims=True)
        return jnp.exp(-(square + head_sq - 2.0 * full_dot_t(parts, heads)) / (2.0 * width))

    same = lax.broadcasted_iota(jnp.int32, (n_heads, n_heads), 0) == lax.broadcasted_iota(
        jnp.int32, (n_heads, n_heads), 1
    )
    block = distances(head_emb, heads) + jnp.where(same, ridge_ref[0], 0.0)
    kept = panel_ref.shape[0]
    head = lax.broadcasted_iota(jnp.int32, (CHUNK, n_heads), 1)
    head_place = (head % PW >> 3) * kept + (head // PW) * SUB + (head & (SUB - 1))
    local = lax.broadcasted_iota(jnp.int32, (CHUNK, n_heads), 0)

    def chunk(step):
        emb_ref, out_ref, start = (
            (rows_emb_ref, rows_ref, step * CHUNK)
            if step < rows_ref.shape[0] // CHUNK
            else (cols_emb_ref, cols_ref, step * CHUNK - rows_ref.shape[0])
        )
        emb = emb_ref[start : start + CHUNK, :]
        if emb_ref is rows_emb_ref:
            place = place_ref[start // kept] + start % kept + local
        else:
            column = place_ref[2] + start + local
            place = (column >> 3) * kept + place_ref[3] + (column & (SUB - 1))
        base = distances(emb, in_three(emb))
        out_ref[start : start + CHUNK, :] = base + jnp.where(place == head_place, ridge_ref[0], 0.0)

    chunks = (rows_ref.shape[0] + cols_ref.shape[0]) // CHUNK
    groups = PW // SUB

    def between(panel):
        def run(b):
            done = panel * groups + b
            for step in range(done * chunks // (2 * groups), (done + 1) * chunks // (2 * groups)):
                chunk(step)

        return run

    def factor_into(block, out_ref, run):
        inv = inverse_factor([block[SUB * g : SUB * g + SUB] for g in range(groups)], run)
        for g, rows in enumerate(inv):
            out_ref[SUB * g : SUB * g + SUB, :] = rows

    factor_into(block[:PW, :PW], first_ref, between(0))
    corner = dot_t(block[PW:, :PW], first_ref[...])
    factor_into(block[PW:, PW:] - dot_t(corner, corner), second_ref, between(1))

    first, second, below = in_two(first_ref[...]), in_two(second_ref[...]), in_two(corner)

    def panels_of(ref):
        left = split_dot_t(in_two(ref[:, :PW]), first)
        left_two = in_two(left)
        right = split_dot_t(in_two(ref[:, PW:] - split_dot_t(left_two, below)), second)
        return left, right, left_two, in_two(right)

    row_left, row_right, row_left_two, row_right_two = panels_of(rows_ref)
    _, _, col_left_two, col_right_two = panels_of(cols_ref)
    panel_ref[:, :PW] = row_left[:kept]
    panel_ref[:, PW:] = row_right[:kept]

    def rows_of(two, part):
        return two[0][part], two[1][part]

    for out_ref, start in ((given_ref, kept), (mine_ref, 0)):
        part = slice(start, start + kept)
        out_ref[...] = (
            tile_ref[part, :]
            - split_dot_t(rows_of(row_left_two, part), col_left_two)
            - split_dot_t(rows_of(row_right_two, part), col_right_two)
        )


def updated(place, ridge, head_0, head_1, rows_emb, cols_emb, tile):
    kept = rows_emb.shape[0] // 2
    wide = jax.ShapeDtypeStruct((kept, tile.shape[1]), jnp.float32)
    scalar = pl.BlockSpec(memory_space=pltpu.SMEM)
    return pl.pallas_call(
        update_kernel,
        out_shape=(jax.ShapeDtypeStruct((kept, 2 * PW), jnp.float32), wide, wide),
        in_specs=[scalar, scalar] + [pl.BlockSpec(memory_space=pltpu.VMEM)] * 5,
        scratch_shapes=[pltpu.VMEM((PW, PW), jnp.float32)] * 2
        + [pltpu.VMEM((emb.shape[0], 2 * PW), jnp.float32) for emb in (rows_emb, cols_emb)],
        compiler_params=pltpu.CompilerParams(vmem_limit_bytes=32 * 2**20),
        cost_estimate=pl.CostEstimate(flops=900_000_000, bytes_accessed=8_000_000, transcendentals=256),
    )(place, ridge, head_0, head_1, rows_emb, cols_emb, tile)


def take_kernel(start_ref, index_ref, points_ref, emb_ref, own_ref):
    point = lax.broadcasted_iota(jnp.int32, (points_ref.shape[0], index_ref.shape[1]), 0)
    hot = jnp.where(point == index_ref[...] - start_ref[0], 1.0, 0.0).astype(jnp.bfloat16)
    high, middle, low = (
        lax.dot_general(hot, part, (((0,), (0,)), ((), ())), preferred_element_type=jnp.float32)
        for part in in_three(points_ref[...])
    )
    emb_ref[...] = high + middle + low
    own = emb_ref[pl.ds(pl.multiple_of(start_ref[1], SUB), SUB), :]
    for peer in range(own_ref.shape[0]):
        own_ref[peer] = own


def taken_rows(start, index, points, peers):
    width = points.shape[1]
    vmem = pl.BlockSpec(memory_space=pltpu.VMEM)
    return pl.pallas_call(
        take_kernel,
        out_shape=(
            jax.ShapeDtypeStruct((index.shape[0], width), jnp.float32),
            jax.ShapeDtypeStruct((peers, SUB, width), jnp.float32),
        ),
        in_specs=[pl.BlockSpec(memory_space=pltpu.SMEM), vmem, vmem],
        compiler_params=pltpu.CompilerParams(vmem_limit_bytes=20 * 2**20),
        cost_estimate=pl.CostEstimate(flops=600_000_000, bytes_accessed=3_000_000, transcendentals=0),
    )(start, index[None, :], points)


def chosen(*values):
    slots = lax.iota(jnp.int32, len(values))
    table = jnp.zeros(len(values), jnp.int32)
    for slot, value in enumerate(values):
        table = jnp.where(slots == slot, value, table)
    return table


def per_device(points, landmark_index, targets, ridge_shift):
    rows_here = landmark_index.shape[0]
    block_points = points.shape[0]
    row_pos = lax.axis_index(ROWS)
    col_pos = lax.axis_index("cols")
    y_pos = lax.axis_index(Y)
    n_rows = lax.axis_size(ROWS)
    n_y = lax.axis_size(Y)
    per_y = n_rows // n_y
    quarter = C // 2 // n_rows
    half = C // 4
    half_pos = lax.axis_index("half")
    upper = half_pos == 1
    ridge = ridge_shift[0]
    across = [(y, n_y - 1 - y) for y in range(n_y)]
    swap = [(0, 1), (1, 0)]

    def ordered(flag, mine, other, axis):
        return jnp.concatenate([jnp.where(flag, other, mine), jnp.where(flag, mine, other)], axis=axis)

    n_z = lax.axis_size("z")
    start = chosen(row_pos * block_points, col_pos * quarter, half_pos * half)
    embedded, own_copies = taken_rows(start, landmark_index, points, n_z)
    peer_embedded = lax.ppermute(embedded, Y, across)
    own_line = lax.all_to_all(own_copies, "z", 0, 0, tiled=True)
    column_emb = lax.optimization_barrier(to_all(own_line, NEAR).reshape(half, -1))
    own_targets = jnp.concatenate([targets, lax.ppermute(targets, Y, across)], axis=0)
    peer_targets = lax.ppermute(own_targets, "cols", swap)
    pair_targets = lax.optimization_barrier(ordered(col_pos == 1, own_targets, peer_targets, 1))
    peer_pos = row_pos + (n_y - 1 - 2 * y_pos) * per_y
    places = chosen(row_pos * rows_here, peer_pos * rows_here, half_pos * half, col_pos * quarter)
    rows_emb, places = lax.optimization_barrier(
        (jnp.concatenate([embedded, peer_embedded], axis=0), places)
    )

    rows_sq = squares(rows_emb)
    col_sq = squares(column_emb)
    local = lax.iota(jnp.int32, rows_here)
    row_place = jnp.concatenate([row_pos * rows_here + local, peer_pos * rows_here + local])
    column = half_pos * half + lax.iota(jnp.int32, half)
    col_place = column // quarter * rows_here + col_pos * quarter + column % quarter

    tile = gaussian(rows_emb, rows_sq, column_emb, col_sq)
    tile = lax.optimization_barrier(
        tile + jnp.where(row_place[:, None] == col_place[None, :], ridge, 0.0)
    )
    partial = lax.dot_general(
        pair_targets, tile, (((0,), (0,)), ((), ())), precision=lax.Precision.HIGH, preferred_element_type=jnp.float32
    )
    n_plane = lax.axis_size(PLANE)
    arrived = lax.all_to_all(partial.reshape(n_plane, -1, half), PLANE, 0, 0, tiled=True)
    nearer = arrived.reshape(2, n_plane // 2, -1, half).sum(axis=1)
    joined = jnp.concatenate([nearer[0], nearer[1]], axis=1).reshape(n_z, -1, 2 * half)
    projected = lax.all_to_all(joined, "z", 0, 0, tiled=True).sum(axis=0)

    sent_heads = lax.ppermute(column_emb[:PW], Y, [(y, n_y - 1 - y) for y in range(n_y // 2)])
    own_heads = jnp.where(upper, sent_heads, column_emb[:PW])
    peer_heads = lax.ppermute(own_heads, "cols", swap)
    swapped = col_pos == 1
    head_0 = jnp.where(swapped, peer_heads, own_heads)
    head_1 = jnp.where(swapped, own_heads, peer_heads)

    panels, mine, given = updated(
        places, ridge_shift, head_0, head_1, rows_emb, column_emb, tile
    )
    taken = lax.ppermute(given, Y, across)
    remainder = jnp.concatenate(
        [jnp.where(upper, taken, mine)[:, PW:], jnp.where(upper, mine, taken)], axis=1
    )
    return projected, panels, remainder


def solution(mesh):
    split = Mesh(
        mesh.devices.reshape(2, 2, 4, 8, mesh.shape["cols"]), ("half", "near", "x", "z", "cols")
    )
    placed = (P(ROWS, None), P(ROWS), P(ROWS, "cols"), P())
    return jax.shard_map(
        per_device,
        mesh=split,
        in_specs=placed,
        out_specs=(P(ROWS, "cols"), P(ROWS, None), P(ROWS, "cols")),
        check_vma=False,
    )
```

```python
import jax
import jax.numpy as jnp
from jax import lax
from jax.experimental import pallas as pl
from jax.experimental.pallas import tpu as pltpu
from jax.sharding import Mesh
from jax.sharding import PartitionSpec as P


C = 2048
PW = 128
Y = ("half", "near")
PLANE = ("half", "near", "x")
NEAR = ("near", "x")
ROWS = ("half", "near", "x", "z")
SUB = 8
CHUNK = 128

exact_mode = lax.Precision.HIGHEST


def to_all(x, axis):
    peers = lax.axis_size(axis)
    return lax.all_to_all(jnp.broadcast_to(x[None], (peers, *x.shape)), axis, 0, 0, tiled=True)


def dot_t(left, right):
    return lax.dot_general(
        left, right, (((1,), (1,)), ((), ())), precision=exact_mode, preferred_element_type=jnp.float32
    )


def in_two(x):
    high = x.astype(jnp.bfloat16)
    return high, (x - high.astype(jnp.float32)).astype(jnp.bfloat16)


def split_dot_t(left, right):
    def part(a, b):
        return lax.dot_general(a, b, (((1,), (1,)), ((), ())), preferred_element_type=jnp.float32)

    return part(left[0], right[1]) + part(left[1], right[0]) + part(left[0], right[0])


def gaussian(left, left_sq, right, right_sq):
    cross = dot_t(left, right)
    return jnp.exp(-(left_sq[:, None] + right_sq[None, :] - 2.0 * cross) / (2.0 * left.shape[1]))


def squares(x):
    return jnp.sum(x * x, axis=1)


def inverse_factor(rows, between):
    groups = len(rows)
    ids = lax.broadcasted_iota(jnp.int32, (SUB, PW), 0)
    lanes = lax.broadcasted_iota(jnp.int32, (SUB, PW), 1)
    inv = [jnp.where(lanes == ids + SUB * g, 1.0, 0.0).astype(jnp.float32) for g in range(groups)]
    for b in range(groups):
        cols = [
            [jnp.broadcast_to(rows[i][:, SUB * b + j : SUB * b + j + 1], (SUB, PW)) for i in range(b, groups)]
            for j in range(SUB)
        ]
        head, inv_head = rows[b], inv[b]
        steps = []
        for k in range(SUB):
            spread = [jnp.broadcast_to(cols[k][0][j : j + 1], (SUB, PW)) for j in range(k, SUB)]
            scale = lax.rsqrt(spread[0])
            row = jnp.broadcast_to(head[k : k + 1], (SUB, PW)) * scale
            inv_row = jnp.broadcast_to(inv_head[k : k + 1], (SUB, PW)) * scale
            mult = [c * scale for c in cols[k]]
            mult[0] = jnp.where(ids > k, mult[0], 0.0)
            for j in range(k + 1, SUB):
                there = spread[j - k] * scale
                cols[j] = [c - m * there for c, m in zip(cols[j], mult)]
            head = head - mult[0] * row
            inv_head = jnp.where(ids == k, inv_row, inv_head - mult[0] * inv_row)
            steps.append((row, inv_row, mult))
        inv[b] = inv_head
        for i in range(b + 1, groups):
            for row, inv_row, mult in steps:
                rows[i] = rows[i] - mult[i - b] * row
                inv[i] = inv[i] - mult[i - b] * inv_row
        between(b)
    return inv


def in_three(x):
    high, rest = x.astype(jnp.bfloat16), x
    rest = rest - high.astype(jnp.float32)
    middle = rest.astype(jnp.bfloat16)
    return high, middle, (rest - middle.astype(jnp.float32)).astype(jnp.bfloat16)


def full_dot_t(left, right):
    total = None
    for i, j in ((2, 0), (0, 2), (1, 1), (1, 0), (0, 1), (0, 0)):
        part = lax.dot_general(
            left[i], right[j], (((1,), (1,)), ((), ())), preferred_element_type=jnp.float32
        )
        total = part if total is None else total + part
    return total


def update_kernel(
    place_ref, ridge_ref, head_0_ref, head_1_ref, rows_emb_any, cols_emb_any, tile_any,
    panel_ref, mine_ref, given_ref, first_ref, second_ref, rows_ref, cols_ref,
    rows_emb_ref, cols_emb_ref, tile_ref, rows_sem, cols_sem, tile_sem,
):
    rows_copy = pltpu.make_async_copy(rows_emb_any, rows_emb_ref, rows_sem)
    cols_copy = pltpu.make_async_copy(cols_emb_any, cols_emb_ref, cols_sem)
    tile_copy = pltpu.make_async_copy(tile_any, tile_ref, tile_sem)
    for copy in (rows_copy, cols_copy, tile_copy):
        copy.start()
    head_emb = jnp.concatenate([head_0_ref[...], head_1_ref[...]], axis=0)
    heads = in_three(head_emb)
    n_heads, width = head_emb.shape
    ones = jnp.ones((SUB, width), jnp.bfloat16)
    head_sq = sum(
        lax.dot_general(ones, part, (((1,), (1,)), ((), ())), preferred_element_type=jnp.float32)
        for part in reversed(in_three(head_emb * head_emb))
    )[:1]

    def distances(emb, parts):
        square = jnp.sum(emb * emb, axis=1, keepdims=True)
        return jnp.exp(-(square + head_sq - 2.0 * full_dot_t(parts, heads)) / (2.0 * width))

    same = lax.broadcasted_iota(jnp.int32, (n_heads, n_heads), 0) == lax.broadcasted_iota(
        jnp.int32, (n_heads, n_heads), 1
    )
    block = distances(head_emb, heads) + jnp.where(same, ridge_ref[0], 0.0)
    kept = panel_ref.shape[0]
    head = lax.broadcasted_iota(jnp.int32, (CHUNK, n_heads), 1)
    head_place = (head % PW >> 3) * kept + (head // PW) * SUB + (head & (SUB - 1))
    local = lax.broadcasted_iota(jnp.int32, (CHUNK, n_heads), 0)

    def chunk(step):
        emb_ref, out_ref, start = (
            (rows_emb_ref, rows_ref, step * CHUNK)
            if step < rows_ref.shape[0] // CHUNK
            else (cols_emb_ref, cols_ref, step * CHUNK - rows_ref.shape[0])
        )
        if start == 0:
            (rows_copy if emb_ref is rows_emb_ref else cols_copy).wait()
        emb = emb_ref[start : start + CHUNK, :]
        if emb_ref is rows_emb_ref:
            place = place_ref[start // kept] + start % kept + local
        else:
            column = place_ref[2] + start + local
            place = (column >> 3) * kept + place_ref[3] + (column & (SUB - 1))
        base = distances(emb, in_three(emb))
        out_ref[start : start + CHUNK, :] = base + jnp.where(place == head_place, ridge_ref[0], 0.0)

    chunks = (rows_ref.shape[0] + cols_ref.shape[0]) // CHUNK
    groups = PW // SUB

    def between(panel):
        def run(b):
            done = panel * groups + b
            for step in range(done * chunks // (2 * groups), (done + 1) * chunks // (2 * groups)):
                chunk(step)

        return run

    def factor_into(block, out_ref, run):
        inv = inverse_factor([block[SUB * g : SUB * g + SUB] for g in range(groups)], run)
        for g, rows in enumerate(inv):
            out_ref[SUB * g : SUB * g + SUB, :] = rows

    factor_into(block[:PW, :PW], first_ref, between(0))
    corner = dot_t(block[PW:, :PW], first_ref[...])
    factor_into(block[PW:, PW:] - dot_t(corner, corner), second_ref, between(1))

    first, second, below = in_two(first_ref[...]), in_two(second_ref[...]), in_two(corner)

    def panels_of(ref):
        left = split_dot_t(in_two(ref[:, :PW]), first)
        left_two = in_two(left)
        right = split_dot_t(in_two(ref[:, PW:] - split_dot_t(left_two, below)), second)
        return left, right, left_two, in_two(right)

    row_left, row_right, row_left_two, row_right_two = panels_of(rows_ref)
    _, _, col_left_two, col_right_two = panels_of(cols_ref)
    panel_ref[:, :PW] = row_left[:kept]
    panel_ref[:, PW:] = row_right[:kept]

    def rows_of(two, part):
        return two[0][part], two[1][part]

    tile_copy.wait()
    for out_ref, start in ((given_ref, kept), (mine_ref, 0)):
        part = slice(start, start + kept)
        out_ref[...] = (
            tile_ref[part, :]
            - split_dot_t(rows_of(row_left_two, part), col_left_two)
            - split_dot_t(rows_of(row_right_two, part), col_right_two)
        )


def updated(place, ridge, head_0, head_1, rows_emb, cols_emb, tile):
    kept = rows_emb.shape[0] // 2
    wide = jax.ShapeDtypeStruct((kept, tile.shape[1]), jnp.float32)
    scalar = pl.BlockSpec(memory_space=pltpu.SMEM)
    return pl.pallas_call(
        update_kernel,
        out_shape=(jax.ShapeDtypeStruct((kept, 2 * PW), jnp.float32), wide, wide),
        in_specs=[scalar, scalar]
        + [pl.BlockSpec(memory_space=pltpu.VMEM)] * 2
        + [pl.BlockSpec(memory_space=pl.ANY)] * 3,
        scratch_shapes=[pltpu.VMEM((PW, PW), jnp.float32)] * 2
        + [pltpu.VMEM((emb.shape[0], 2 * PW), jnp.float32) for emb in (rows_emb, cols_emb)]
        + [pltpu.VMEM(whole.shape, jnp.float32) for whole in (rows_emb, cols_emb, tile)]
        + [pltpu.SemaphoreType.DMA(())] * 3,
        cost_estimate=pl.CostEstimate(flops=900_000_000, bytes_accessed=8_000_000, transcendentals=256),
    )(place, ridge, head_0, head_1, rows_emb, cols_emb, tile)


def take_kernel(start_ref, index_ref, points_ref, emb_ref, own_ref):
    point = lax.broadcasted_iota(jnp.int32, (points_ref.shape[0], index_ref.shape[1]), 0)
    hot = jnp.where(point == index_ref[...] - start_ref[0], 1.0, 0.0).astype(jnp.bfloat16)
    high, middle, low = (
        lax.dot_general(hot, part, (((0,), (0,)), ((), ())), preferred_element_type=jnp.float32)
        for part in in_three(points_ref[...])
    )
    emb_ref[...] = high + middle + low
    own = emb_ref[pl.ds(pl.multiple_of(start_ref[1], SUB), SUB), :]
    for peer in range(own_ref.shape[0]):
        own_ref[peer] = own


def taken_rows(start, index, points, peers):
    width = points.shape[1]
    vmem = pl.BlockSpec(memory_space=pltpu.VMEM)
    return pl.pallas_call(
        take_kernel,
        out_shape=(
            jax.ShapeDtypeStruct((index.shape[0], width), jnp.float32),
            jax.ShapeDtypeStruct((peers, SUB, width), jnp.float32),
        ),
        in_specs=[pl.BlockSpec(memory_space=pltpu.SMEM), vmem, vmem],
        compiler_params=pltpu.CompilerParams(vmem_limit_bytes=20 * 2**20),
        cost_estimate=pl.CostEstimate(flops=600_000_000, bytes_accessed=3_000_000, transcendentals=0),
    )(start, index[None, :], points)


def chosen(*values):
    slots = lax.iota(jnp.int32, len(values))
    table = jnp.zeros(len(values), jnp.int32)
    for slot, value in enumerate(values):
        table = jnp.where(slots == slot, value, table)
    return table


def per_device(points, landmark_index, targets, ridge_shift):
    rows_here = landmark_index.shape[0]
    block_points = points.shape[0]
    row_pos = lax.axis_index(ROWS)
    col_pos = lax.axis_index("cols")
    y_pos = lax.axis_index(Y)
    n_rows = lax.axis_size(ROWS)
    n_y = lax.axis_size(Y)
    per_y = n_rows // n_y
    quarter = C // 2 // n_rows
    half = C // 4
    half_pos = lax.axis_index("half")
    upper = half_pos == 1
    ridge = ridge_shift[0]
    across = [(y, n_y - 1 - y) for y in range(n_y)]
    swap = [(0, 1), (1, 0)]

    def ordered(flag, mine, other, axis):
        return jnp.concatenate([jnp.where(flag, other, mine), jnp.where(flag, mine, other)], axis=axis)

    n_z = lax.axis_size("z")
    start = chosen(row_pos * block_points, col_pos * quarter, half_pos * half)
    embedded, own_copies = taken_rows(start, landmark_index, points, n_z)
    peer_embedded = lax.ppermute(embedded, Y, across)
    own_line = lax.all_to_all(own_copies, "z", 0, 0, tiled=True)
    column_emb = lax.optimization_barrier(to_all(own_line, NEAR).reshape(half, -1))
    own_targets = jnp.concatenate([targets, lax.ppermute(targets, Y, across)], axis=0)
    peer_targets = lax.ppermute(own_targets, "cols", swap)
    pair_targets = lax.optimization_barrier(ordered(col_pos == 1, own_targets, peer_targets, 1))
    peer_pos = row_pos + (n_y - 1 - 2 * y_pos) * per_y
    places = chosen(row_pos * rows_here, peer_pos * rows_here, half_pos * half, col_pos * quarter)
    rows_emb, places = lax.optimization_barrier(
        (jnp.concatenate([embedded, peer_embedded], axis=0), places)
    )

    rows_sq = squares(rows_emb)
    col_sq = squares(column_emb)
    local = lax.iota(jnp.int32, rows_here)
    row_place = jnp.concatenate([row_pos * rows_here + local, peer_pos * rows_here + local])
    column = half_pos * half + lax.iota(jnp.int32, half)
    col_place = column // quarter * rows_here + col_pos * quarter + column % quarter

    tile = gaussian(rows_emb, rows_sq, column_emb, col_sq)
    tile = lax.optimization_barrier(
        tile + jnp.where(row_place[:, None] == col_place[None, :], ridge, 0.0)
    )
    partial = lax.dot_general(
        pair_targets, tile, (((0,), (0,)), ((), ())), precision=lax.Precision.HIGH, preferred_element_type=jnp.float32
    )
    n_plane = lax.axis_size(PLANE)
    arrived = lax.all_to_all(partial.reshape(n_plane, -1, half), PLANE, 0, 0, tiled=True)
    nearer = arrived.reshape(2, n_plane // 2, -1, half).sum(axis=1)
    joined = jnp.concatenate([nearer[0], nearer[1]], axis=1).reshape(n_z, -1, 2 * half)
    projected = lax.all_to_all(joined, "z", 0, 0, tiled=True).sum(axis=0)

    sent_heads = lax.ppermute(column_emb[:PW], Y, [(y, n_y - 1 - y) for y in range(n_y // 2)])
    own_heads = jnp.where(upper, sent_heads, column_emb[:PW])
    peer_heads = lax.ppermute(own_heads, "cols", swap)
    swapped = col_pos == 1
    head_0 = jnp.where(swapped, peer_heads, own_heads)
    head_1 = jnp.where(swapped, own_heads, peer_heads)

    panels, mine, given = updated(places, ridge_shift, head_0, head_1, rows_emb, column_emb, tile)
    taken = lax.ppermute(given, Y, across)
    remainder = jnp.concatenate(
        [jnp.where(upper, taken, mine)[:, PW:], jnp.where(upper, mine, taken)], axis=1
    )
    return projected, panels, remainder


def solution(mesh):
    split = Mesh(
        mesh.devices.reshape(2, 2, 4, 8, mesh.shape["cols"]), ("half", "near", "x", "z", "cols")
    )
    placed = (P(ROWS, None), P(ROWS), P(ROWS, "cols"), P())
    return jax.shard_map(
        per_device,
        mesh=split,
        in_specs=placed,
        out_specs=(P(ROWS, "cols"), P(ROWS, None), P(ROWS, "cols")),
        check_vma=False,
    )
```
